32 devices in a mesh: rows: 8 (over y, x, core), model: 4 (over z).
Axes of the slice: x: 2, y: 2, z: 4, core: 2. Of those that a mesh axis runs over, the one named last changes fastest.
Arguments:
- one_query: float32 [5120, 5120], P('rows', 'model'), may hold values from -0.125 to 0.125
- other_query: float32 [5120, 5120], P('rows', 'model'), may hold values from -0.078125 to 0.078125
- one_key: float32 [5120, 5120], P('rows', 'model'), may hold values from -0.125 to 0.125
- other_key: float32 [5120, 5120], P('rows', 'model'), may hold values from -0.078125 to 0.078125
- one_value: float32 [5120, 5120], P('rows', 'model'), may hold values from -0.125 to 0.125
- other_value: float32 [5120, 5120], P('rows', 'model'), may hold values from -0.078125 to 0.078125
- mix_share: float32 [5120], P('rows'), may hold values from 0.2 to 0.8
- norm_gain: float32 [5120], P('rows'), may hold values from 0.25 to 1.75
Outputs:
- final_query: bfloat16 [5120, 5120], P(None, 'model')
- final_key: bfloat16 [5120, 5120], P(None, 'model')
- final_value: bfloat16 [5120, 5120], P(None, 'model')
- factor_query: float32 [5120], P('model')
- factor_key: float32 [5120], P('model')
- factor_value: float32 [5120], P('model')
The draws below stay inside these ranges and needn't reach their ends.
All inputs are finite; a program needn't handle non-finite values. Where the reference program divides by a largest or mean magnitude, that divisor is 1e-20 or more.
Results may differ from the reference program's by a relative error of at most 0.001.
Values may be sent and summed in bfloat16 or wider, within the bound.
A program may use at most 192 MiB of HBM per device.

```python
import jax
import jax.numpy as jnp

D_MODEL = 5120
Q_DIM = 5120
KV_DIM = 5120


def raised(array, stream_key, source, target, blocks, factor):
    def block_of(position):
        return (jnp.arange(array.shape[position]) // (array.shape[position] // blocks)).reshape((-1,) + (1,) * (array.ndim - 1 - position))

    near = jax.random.permutation(stream_key, blocks)[block_of(target)]
    far = (block_of(target) + blocks // 2) % blocks
    return jnp.where((block_of(source) == near) | (block_of(source) == far), factor * array, array)


def level_of(rng, dims, pieces, least, high):
    gain = 1.0
    for position, blocks in pieces:
        draws = jax.random.uniform(jax.random.fold_in(jax.random.fold_in(rng, 6), position), (blocks,), jnp.float32, least / len(pieces), high / len(pieces))
        gain = gain * jnp.repeat(jnp.exp(draws), dims[position] // blocks).reshape((-1,) + (1,) * (len(dims) - 1 - position))
    return gain


def normal_values(rng, dims, spread, bound, split=(), kind=jnp.bfloat16):
    level = level_of(rng, dims, split, -0.22, 0.18) if split else 1.0
    result = jax.random.normal(rng, dims, jnp.float32) * spread * level
    return jnp.minimum(jnp.maximum(result, -bound), bound).astype(kind)


def noise_with(rng, dims, deviation, most, split, heavy, kind=jnp.bfloat16):
    entries = deviation * jax.random.normal(rng, dims, jnp.float32)
    if split:
        entries = entries * level_of(rng, dims, split, -0.22, 0.18)
    return jnp.clip(raised(entries, jax.random.fold_in(rng, 3), *heavy), -most, most).astype(kind)


def setup_inputs(seed: int = 0) -> dict:
    arg_keys = jax.random.split(jax.random.key(seed), 9)
    return {
        "one_query": noise_with(arg_keys[0], (D_MODEL, Q_DIM), D_MODEL ** -0.5, 0.125, ((0, 8), (1, 4)), (0, 1, 8, 2.0), jnp.float32),
        "other_query": normal_values(arg_keys[1], (D_MODEL, Q_DIM), D_MODEL ** -0.5, 0.078125, ((0, 8), (1, 4)), jnp.float32),
        "one_key": noise_with(arg_keys[2], (D_MODEL, KV_DIM), D_MODEL ** -0.5, 0.125, ((0, 8), (1, 4)), (0, 1, 8, 2.0), jnp.float32),
        "other_key": normal_values(arg_keys[3], (D_MODEL, KV_DIM), D_MODEL ** -0.5, 0.078125, ((0, 8), (1, 4)), jnp.float32),
        "one_value": noise_with(arg_keys[4], (D_MODEL, KV_DIM), D_MODEL ** -0.5, 0.125, ((0, 8), (1, 4)), (0, 1, 8, 2.0), jnp.float32),
        "other_value": normal_values(arg_keys[5], (D_MODEL, KV_DIM), D_MODEL ** -0.5, 0.078125, ((0, 8), (1, 4)), jnp.float32),
        "mix_share": jnp.clip(0.2 + 0.6 * jax.random.uniform(arg_keys[6], (D_MODEL,), jnp.float32) ** level_of(arg_keys[6], (D_MODEL,), ((0, 8),), -0.2, 0.2), 0.2, 0.8),
        "norm_gain": jnp.clip(1.0 + 0.15 * jax.random.normal(arg_keys[7], (D_MODEL,), jnp.float32), 0.25, 1.75),
    }


def reference(one_query, other_query, one_key, other_key, one_value, other_value, mix_share, norm_gain):
    result_query = mix_share[:, None] * one_query + (1.0 - mix_share[:, None]) * other_query
    result_key = mix_share[:, None] * one_key + (1.0 - mix_share[:, None]) * other_key
    result_value = mix_share[:, None] * one_value + (1.0 - mix_share[:, None]) * other_value
    result_gained_query = result_query * norm_gain[:, None]
    result_gained_key = result_key * norm_gain[:, None]
    result_gained_value = result_value * norm_gain[:, None]
    factor_query = jnp.max(jnp.abs(result_gained_query), axis=0)
    final_query = (result_gained_query / factor_query).astype(jnp.bfloat16)
    factor_key = jnp.max(jnp.abs(result_gained_key), axis=0)
    final_key = (result_gained_key / factor_key).astype(jnp.bfloat16)
    factor_value = jnp.max(jnp.abs(result_gained_value), axis=0)
    final_value = (result_gained_value / factor_value).astype(jnp.bfloat16)
    return final_query, final_key, final_value, factor_query, factor_key, factor_value
```

```python
import functools

import jax
import jax.numpy as jnp
from jax import lax
from jax.experimental import pallas as pl
from jax.experimental.pallas import tpu as pltpu
from jax.sharding import PartitionSpec as P

MESH = pl.DeviceIdType.MESH
LANES = 128
IN_VMEM = 0
OWN_X, OWN_Y, OWN_S, DIAG, X_S, Y_S, D_S = range(7)


def gathered_by_collectives(one_query, other_query, one_key, other_key, one_value, other_value, mix_share, norm_gain):
    share, gain = mix_share[:, None], norm_gain[:, None]
    gained = [
        (share * one + (1.0 - share) * other) * gain
        for one, other in ((one_query, other_query), (one_key, other_key), (one_value, other_value))
    ]
    factors = lax.pmax(tuple(jnp.max(jnp.abs(g), axis=0) for g in gained), "rows")
    narrow = [(g / f).astype(jnp.bfloat16) for g, f in zip(gained, factors)]
    return (*(lax.all_gather(w, "rows", axis=0, tiled=True) for w in narrow), *factors)


def kernel(chunks, share, gain, *refs):
    args, outs, factors = refs[0:6], refs[6:9], refs[9:12]
    (held, wide_one, wide_other, box_first, box_rest, staged,
     load_sem, send_sem, bulk_sem, x_sem, y_sem, d_sem, box_sem, keep_sem) = refs[12:]
    rows, columns = args[0].shape
    height = rows // chunks
    half = chunks // 2
    tiles = columns // LANES

    me = lax.axis_index("rows")
    core, east, north = lax.rem(me, 2), lax.rem(me // 2, 2), me // 4

    def peer(d):
        return (
            lax.rem(north + d // 4, 2) * 4
            + lax.rem(east + (d // 2) % 2, 2) * 2
            + lax.rem(core + d % 2, 2)
        )

    sibling, at_x, at_y, at_d = peer(1), peer(2), peer(4), peer(6)

    loads = [pltpu.make_async_copy(args[i], held.at[i], load_sem.at[i]) for i in range(6)]
    for load in loads:
        load.start()

    barrier = pltpu.get_barrier_semaphore()
    for d in range(1, 8):
        pl.semaphore_signal(barrier, inc=1, device_id={"rows": peer(d)}, device_id_type=MESH)

    for j in range(rows // LANES):
        s = jnp.broadcast_to(share[:, j * LANES:(j + 1) * LANES], (LANES, LANES)).T
        g = jnp.broadcast_to(gain[:, j * LANES:(j + 1) * LANES], (LANES, LANES)).T
        wide_one[j * LANES:(j + 1) * LANES, :] = s * g
        wide_other[j * LANES:(j + 1) * LANES, :] = (1.0 - s) * g

    def mix(m):
        loads[2 * m].wait()
        loads[2 * m + 1].wait()

        def body(i, top):
            at = pl.ds(pl.multiple_of(i * 8, 8), 8)
            a = jnp.concatenate([wide_one[at, :]] * tiles, axis=1)
            b = jnp.concatenate([wide_other[at, :]] * tiles, axis=1)
            mixed = a * held[2 * m, at, :] + b * held[2 * m + 1, at, :]
            held[2 * m, at, :] = mixed
            return jnp.maximum(top, jnp.abs(mixed))

        top = lax.fori_loop(0, rows // 8, body, jnp.zeros((8, columns), jnp.float32), unroll=4)
        return jnp.max(top, axis=0, keepdims=True)

    def exchange(box, which):
        return [
            pltpu.make_async_remote_copy(
                box.at[me], box.at[me], box_sem.at[2 * which], box_sem.at[2 * which + 1],
                device_id={"rows": peer(d)}, device_id_type=MESH,
            )
            for d in range(1, 8)
        ]

    def exchanged(box, which):
        return pltpu.make_async_remote_copy(
            box.at[pl.ds(0, 7)], box.at[pl.ds(0, 7)], box_sem.at[2 * which], box_sem.at[2 * which + 1],
            device_id={"rows": sibling}, device_id_type=MESH,
        )

    def piece(m, owner, k):
        return outs[m].at[pl.ds(pl.multiple_of(owner * rows + k * height, 16), height), :]

    def copy(m, owner, k, stream, target):
        ref = piece(m, owner, k)
        source = ref
        if m >= IN_VMEM and stream in (OWN_X, OWN_Y, OWN_S):
            source = staged.at[m - IN_VMEM, pl.ds(k * height, height), :]
        arrive = {OWN_X: x_sem, OWN_Y: y_sem, DIAG: d_sem}.get(stream)
        arrive = bulk_sem.at[m, stream] if arrive is None else arrive.at[m, k]
        return pltpu.make_async_remote_copy(
            source, ref, send_sem.at[m, stream], arrive,
            device_id={"rows": target}, device_id_type=MESH,
        )

    def whole(m, stream):
        ref = outs[m].at[pl.ds(0, rows), :]
        return pltpu.make_async_remote_copy(
            ref, ref, send_sem.at[m, stream], bulk_sem.at[m, stream],
            device_id={"rows": sibling}, device_id_type=MESH,
        )

    def narrow(m, k, inverse):
        def body(i, _):
            at = pl.multiple_of(k * height + i * 16, 16)
            small = (held[2 * m, pl.ds(at, 16), :] * inverse).astype(jnp.bfloat16)
            if m < IN_VMEM:
                outs[m][pl.ds(pl.multiple_of(me * rows + at, 16), 16), :] = small
            else:
                staged[m - IN_VMEM, pl.ds(at, 16), :] = small
            return 0

        lax.fori_loop(0, height // 16, body, 0, unroll=True)

    def send_own(m, k):
        copy(m, me, k, OWN_X, at_x).start()
        copy(m, me, k, OWN_Y, at_y).start()
        copy(m, me, k, OWN_S, sibling).start()

    box_first[me] = mix(0)
    pl.semaphore_wait(barrier, 7)
    for c in exchange(box_first, 0):
        c.start()
    exchanged(box_first, 0).wait_recv()
    factor = jnp.max(box_first[...], axis=0)
    factors[0][...] = factor
    inverse = 1.0 / factor
    for k in range(chunks):
        narrow(0, k, inverse)
        if 1 <= k <= half:
            send_own(0, k - 1)

    box_rest[me, 0:1] = mix(1)
    box_rest[me, 1:2] = mix(2)
    for c in exchange(box_rest, 1):
        c.start()
    for k in range(half, chunks):
        send_own(0, k)
    exchanged(box_rest, 1).wait_recv()
    both = jnp.max(box_rest[...], axis=0)
    for m in (1, 2):
        factor = both[m - 1:m]
        factors[m][...] = factor
        inverse = 1.0 / factor
        for k in range(chunks):
            narrow(m, k, inverse)
            if k:
                send_own(m, k - 1)
        send_own(m, chunks - 1)
    kept = [
        pltpu.make_async_copy(
            staged.at[m - IN_VMEM],
            outs[m].at[pl.ds(pl.multiple_of(me * rows, 16), rows), :],
            keep_sem.at[m],
        )
        for m in range(IN_VMEM, 3)
    ]
    for keep in kept:
        keep.start()

    for m in range(3):
        for k in range(chunks):
            copy(m, at_x, k, OWN_X, at_x).wait_recv()
            copy(m, at_x, k, X_S, sibling).start()
            if k < half:
                copy(m, at_x, k, DIAG, at_y).start()
            copy(m, at_y, k, OWN_Y, at_y).wait_recv()
            copy(m, at_y, k, Y_S, sibling).start()
            if k >= half:
                copy(m, at_y, k, DIAG, at_x).start()
    for m in range(3):
        for k in range(half):
            for part in (k, k + half):
                copy(m, at_d, part, DIAG, at_y).wait_recv()
                copy(m, at_d, part, D_S, sibling).start()

    for m in range(3):
        for stream in (OWN_S, X_S, Y_S, D_S):
            whole(m, stream).wait_recv()
    for m in range(3):
        for stream in range(7):
            whole(m, stream).wait_send()
    for keep in kept:
        keep.wait()
    exchanged(box_first, 0).wait_send()
    exchanged(box_rest, 1).wait_send()


def gathered_by_kernel(*arrays):
    *weights, mix_share, norm_gain = arrays
    rows, columns = weights[0].shape
    chunks = 8
    vmem, hbm = pl.BlockSpec(memory_space=pltpu.VMEM), pl.BlockSpec(memory_space=pltpu.HBM)
    dma = pltpu.SemaphoreType.DMA
    results = pl.pallas_call(
        functools.partial(kernel, chunks),
        out_shape=[pltpu.VMEM((8 * rows, columns), jnp.bfloat16)] * IN_VMEM
        + [jax.ShapeDtypeStruct((8 * rows, columns), jnp.bfloat16)] * (3 - IN_VMEM)
        + [jax.ShapeDtypeStruct((1, columns), jnp.float32)] * 3,
        in_specs=[vmem] * 2 + [hbm] * 6,
        out_specs=[vmem] * IN_VMEM + [hbm] * (3 - IN_VMEM) + [vmem] * 3,
        scratch_shapes=[
            pltpu.VMEM((6, rows, columns), jnp.float32),
            pltpu.VMEM((rows, LANES), jnp.float32),
            pltpu.VMEM((rows, LANES), jnp.float32),
            pltpu.VMEM((8, 1, columns), jnp.float32),
            pltpu.VMEM((8, 2, columns), jnp.float32),
            pltpu.VMEM((max(3 - IN_VMEM, 1), rows, columns), jnp.bfloat16),
            dma((6,)),
            dma((3, 7)),
            dma((3, 7)),
            dma((3, chunks)),
            dma((3, chunks)),
            dma((3, chunks)),
            dma((4,)),
            dma((3,)),
        ],
        compiler_params=pltpu.CompilerParams(
            collective_id=0, has_side_effects=True, vmem_limit_bytes=26 * 2**20
        ),
    )(mix_share[None], norm_gain[None], *weights)
    return (*results[:3], *(f[0] for f in results[3:]))


def solution(mesh):
    placed = (P("rows", "model"),) * 6 + (P("rows"),) * 2
    local = gathered_by_kernel if mesh.shape["rows"] == 8 else gathered_by_collectives
    return jax.shard_map(
        local,
        mesh=mesh,
        in_specs=placed,
        out_specs=(P(None, "model"),) * 3 + (P("model"),) * 3,
        check_vma=False,
    )
```

```python
import functools

import jax
import jax.numpy as jnp
from jax import lax
from jax.experimental import pallas as pl
from jax.experimental.pallas import tpu as pltpu
from jax.sharding import PartitionSpec as P

MESH = pl.DeviceIdType.MESH
LANES = 128
OWN_X, OWN_Y, OWN_S, DIAG, X_S, Y_S, D_S = range(7)


def gathered_by_collectives(one_query, other_query, one_key, other_key, one_value, other_value, mix_share, norm_gain):
    share, gain = mix_share[:, None], norm_gain[:, None]
    gained = [
        (share * one + (1.0 - share) * other) * gain
        for one, other in ((one_query, other_query), (one_key, other_key), (one_value, other_value))
    ]
    factors = lax.pmax(tuple(jnp.max(jnp.abs(g), axis=0) for g in gained), "rows")
    narrow = [(g / f).astype(jnp.bfloat16) for g, f in zip(gained, factors)]
    return (*(lax.all_gather(w, "rows", axis=0, tiled=True) for w in narrow), *factors)


def kernel(chunks, share, gain, *refs):
    args, factors = refs[0:6], refs[6]
    outs = [refs[7].at[m] for m in range(3)]
    (held, wide_one, wide_other, box_first, box_rest,
     load_sem, send_sem, bulk_sem, x_sem, y_sem, d_sem, box_sem) = refs[8:]
    rows, columns = args[0].shape
    height = rows // chunks
    half = chunks // 2
    tiles = columns // LANES

    me = lax.axis_index("rows")
    core, east, north = lax.rem(me, 2), lax.rem(me // 2, 2), me // 4

    def peer(d):
        return (
            lax.rem(north + d // 4, 2) * 4
            + lax.rem(east + (d // 2) % 2, 2) * 2
            + lax.rem(core + d % 2, 2)
        )

    sibling, at_x, at_y, at_d = peer(1), peer(2), peer(4), peer(6)

    loads = [pltpu.make_async_copy(args[i], held.at[i], load_sem.at[i]) for i in range(6)]
    for load in loads:
        load.start()

    barrier = pltpu.get_barrier_semaphore()
    for d in range(1, 8):
        pl.semaphore_signal(barrier, inc=1, device_id={"rows": peer(d)}, device_id_type=MESH)

    for j in range(rows // LANES):
        s = jnp.broadcast_to(share[:, j * LANES:(j + 1) * LANES], (LANES, LANES)).T
        g = jnp.broadcast_to(gain[:, j * LANES:(j + 1) * LANES], (LANES, LANES)).T
        wide_one[j * LANES:(j + 1) * LANES, :] = s * g
        wide_other[j * LANES:(j + 1) * LANES, :] = (1.0 - s) * g

    def mix(m):
        loads[2 * m].wait()
        loads[2 * m + 1].wait()

        def body(i, top):
            at = pl.ds(pl.multiple_of(i * 8, 8), 8)
            a = jnp.concatenate([wide_one[at, :]] * tiles, axis=1)
            b = jnp.concatenate([wide_other[at, :]] * tiles, axis=1)
            mixed = a * held[2 * m, at, :] + b * held[2 * m + 1, at, :]
            held[2 * m, at, :] = mixed
            return jnp.maximum(top, jnp.abs(mixed))

        top = lax.fori_loop(0, rows // 8, body, jnp.zeros((8, columns), jnp.float32), unroll=4)
        return jnp.max(top, axis=0, keepdims=True)

    def exchange(box, which):
        return [
            pltpu.make_async_remote_copy(
                box.at[me], box.at[me], box_sem.at[2 * which], box_sem.at[2 * which + 1],
                device_id={"rows": peer(d)}, device_id_type=MESH,
            )
            for d in range(1, 8)
        ]

    def exchanged(box, which):
        return pltpu.make_async_remote_copy(
            box.at[pl.ds(0, 7)], box.at[pl.ds(0, 7)], box_sem.at[2 * which], box_sem.at[2 * which + 1],
            device_id={"rows": sibling}, device_id_type=MESH,
        )

    def piece(m, owner, k):
        return outs[m].at[pl.ds(pl.multiple_of(owner * rows + k * height, 16), height), :]

    def copy(m, owner, k, stream, target):
        ref = piece(m, owner, k)
        arrive = {OWN_X: x_sem, OWN_Y: y_sem, DIAG: d_sem}.get(stream)
        arrive = bulk_sem.at[m, stream] if arrive is None else arrive.at[m, k]
        return pltpu.make_async_remote_copy(
            ref, ref, send_sem.at[m, stream], arrive,
            device_id={"rows": target}, device_id_type=MESH,
        )

    def whole(m, stream):
        ref = outs[m].at[pl.ds(0, rows), :]
        return pltpu.make_async_remote_copy(
            ref, ref, send_sem.at[m, stream], bulk_sem.at[m, stream],
            device_id={"rows": sibling}, device_id_type=MESH,
        )

    def narrow(m, k, inverse):
        def body(i, _):
            at = pl.multiple_of(k * height + i * 16, 16)
            small = (held[2 * m, pl.ds(at, 16), :] * inverse).astype(jnp.bfloat16)
            outs[m][pl.ds(pl.multiple_of(me * rows + at, 16), 16), :] = small
            return 0

        lax.fori_loop(0, height // 16, body, 0, unroll=True)

    def send_own(m, k):
        copy(m, me, k, OWN_X, at_x).start()
        copy(m, me, k, OWN_Y, at_y).start()
        copy(m, me, k, OWN_S, sibling).start()

    box_first[me] = mix(0)
    pl.semaphore_wait(barrier, 7)
    for c in exchange(box_first, 0):
        c.start()
    exchanged(box_first, 0).wait_recv()
    factor = jnp.max(box_first[...], axis=0)
    factors[0] = factor
    inverse = 1.0 / factor
    for k in range(chunks):
        narrow(0, k, inverse)
        if 1 <= k <= half:
            send_own(0, k - 1)

    box_rest[me, 0:1] = mix(1)
    box_rest[me, 1:2] = mix(2)
    for c in exchange(box_rest, 1):
        c.start()
    for k in range(half, chunks):
        send_own(0, k)
    exchanged(box_rest, 1).wait_recv()
    both = jnp.max(box_rest[...], axis=0)
    for m in (1, 2):
        factor = both[m - 1:m]
        factors[m] = factor
        inverse = 1.0 / factor
        for k in range(chunks):
            narrow(m, k, inverse)
            if k:
                send_own(m, k - 1)
        send_own(m, chunks - 1)

    for m in range(3):
        for k in range(chunks):
            copy(m, at_x, k, OWN_X, at_x).wait_recv()
            copy(m, at_x, k, X_S, sibling).start()
            if k < half:
                copy(m, at_x, k, DIAG, at_y).start()
            copy(m, at_y, k, OWN_Y, at_y).wait_recv()
            copy(m, at_y, k, Y_S, sibling).start()
            if k >= half:
                copy(m, at_y, k, DIAG, at_x).start()
    for m in range(3):
        for k in range(half):
            for part in (k, k + half):
                copy(m, at_d, part, DIAG, at_y).wait_recv()
                copy(m, at_d, part, D_S, sibling).start()

    for m in range(3):
        for stream in (OWN_S, X_S, Y_S, D_S):
            whole(m, stream).wait_recv()
    for m in range(3):
        for stream in range(7):
            whole(m, stream).wait_send()
    exchanged(box_first, 0).wait_send()
    exchanged(box_rest, 1).wait_send()


def settle(factors, gathered, *refs):
    targets, sems = refs[:6], refs[6]
    copies = [pltpu.make_async_copy(gathered.at[m], targets[m], sems.at[m]) for m in range(3)]
    for c in copies:
        c.start()
    for m in range(3):
        targets[3 + m][...] = factors[m, 0]
    for c in copies:
        c.wait()


def gathered_by_kernel(*arrays):
    *weights, mix_share, norm_gain = arrays
    rows, columns = weights[0].shape
    chunks = 8
    vmem, hbm = pl.BlockSpec(memory_space=pltpu.VMEM), pl.BlockSpec(memory_space=pltpu.HBM)
    dma = pltpu.SemaphoreType.DMA
    results = pl.pallas_call(
        functools.partial(kernel, chunks),
        out_shape=[
            pltpu.VMEM((3, 1, columns), jnp.float32),
            pltpu.VMEM((3, 8 * rows, columns), jnp.bfloat16),
        ],
        in_specs=[vmem] * 2 + [hbm] * 6,
        out_specs=[vmem] * 2,
        scratch_shapes=[
            pltpu.VMEM((6, rows, columns), jnp.float32),
            pltpu.VMEM((rows, LANES), jnp.float32),
            pltpu.VMEM((rows, LANES), jnp.float32),
            pltpu.VMEM((8, 1, columns), jnp.float32),
            pltpu.VMEM((8, 2, columns), jnp.float32),
            dma((6,)),
            dma((3, 7)),
            dma((3, 7)),
            dma((3, chunks)),
            dma((3, chunks)),
            dma((3, chunks)),
            dma((4,)),
        ],
        compiler_params=pltpu.CompilerParams(
            collective_id=0, has_side_effects=True, vmem_limit_bytes=22 * 2**20
        ),
    )(mix_share[None], norm_gain[None], *weights)
    results = [pltpu.with_memory_space_constraint(r, pltpu.VMEM) for r in results]
    return tuple(
        pl.pallas_call(
            settle,
            out_shape=[jax.ShapeDtypeStruct((8 * rows, columns), jnp.bfloat16)] * 3
            + [jax.ShapeDtypeStruct((columns,), jnp.float32)] * 3,
            in_specs=[vmem] * 2,
            out_specs=[pl.BlockSpec(memory_space=pl.ANY)] * 3 + [vmem] * 3,
            scratch_shapes=[dma((3,))],
            compiler_params=pltpu.CompilerParams(vmem_limit_bytes=2**20),
        )(*results)
    )


def solution(mesh):
    placed = (P("rows", "model"),) * 6 + (P("rows"),) * 2
    local = gathered_by_kernel if mesh.shape["rows"] == 8 else gathered_by_collectives
    return jax.shard_map(
        local,
        mesh=mesh,
        in_specs=placed,
        out_specs=(P(None, "model"),) * 3 + (P("model"),) * 3,
        check_vma=False,
    )
```

```python
import functools

import jax
import jax.numpy as jnp
from jax import lax
from jax.experimental import pallas as pl
from jax.experimental.pallas import tpu as pltpu
from jax.sharding import PartitionSpec as P

MESH = pl.DeviceIdType.MESH
LANES = 128
OWN_X, OWN_Y, OWN_S, DIAG, X_S, Y_S, D_S = range(7)


def gathered_by_collectives(one_query, other_query, one_key, other_key, one_value, other_value, mix_share, norm_gain):
    share, gain = mix_share[:, None], norm_gain[:, None]
    gained = [
        (share * one + (1.0 - share) * other) * gain
        for one, other in ((one_query, other_query), (one_key, other_key), (one_value, other_value))
    ]
    factors = lax.pmax(tuple(jnp.max(jnp.abs(g), axis=0) for g in gained), "rows")
    narrow = [(g / f).astype(jnp.bfloat16) for g, f in zip(gained, factors)]
    return (*(lax.all_gather(w, "rows", axis=0, tiled=True) for w in narrow), *factors)


def kernel(chunks, share, gain, *refs):
    args, factors = refs[0:6], refs[6]
    outs = [refs[7].at[m] for m in range(3)]
    (held, wide_one, wide_other, box_first, box_rest,
     load_sem, send_sem, bulk_sem, x_sem, y_sem, d_sem, box_sem) = refs[8:]
    rows, columns = args[0].shape
    height = rows // chunks
    half = chunks // 2
    tiles = columns // LANES

    me = lax.axis_index("rows")
    core, east, north = lax.rem(me, 2), lax.rem(me // 2, 2), me // 4

    def peer(d):
        return (
            lax.rem(north + d // 4, 2) * 4
            + lax.rem(east + (d // 2) % 2, 2) * 2
            + lax.rem(core + d % 2, 2)
        )

    sibling, at_x, at_y, at_d = peer(1), peer(2), peer(4), peer(6)

    loads = [pltpu.make_async_copy(args[i], held.at[i], load_sem.at[i]) for i in range(6)]
    for load in loads:
        load.start()

    barrier = pltpu.get_barrier_semaphore()
    for d in range(1, 8):
        pl.semaphore_signal(barrier, inc=1, device_id={"rows": peer(d)}, device_id_type=MESH)

    for j in range(rows // LANES):
        s = jnp.broadcast_to(share[j * LANES:(j + 1) * LANES][None], (LANES, LANES)).T
        g = jnp.broadcast_to(gain[j * LANES:(j + 1) * LANES][None], (LANES, LANES)).T
        wide_one[j * LANES:(j + 1) * LANES, :] = s * g
        wide_other[j * LANES:(j + 1) * LANES, :] = (1.0 - s) * g

    def mix(m):
        loads[2 * m].wait()
        loads[2 * m + 1].wait()

        def body(i, top):
            at = pl.ds(pl.multiple_of(i * 8, 8), 8)
            a = jnp.concatenate([wide_one[at, :]] * tiles, axis=1)
            b = jnp.concatenate([wide_other[at, :]] * tiles, axis=1)
            mixed = a * held[2 * m, at, :] + b * held[2 * m + 1, at, :]
            held[2 * m, at, :] = mixed
            return jnp.maximum(top, jnp.abs(mixed))

        top = lax.fori_loop(0, rows // 8, body, jnp.zeros((8, columns), jnp.float32), unroll=4)
        return jnp.max(top, axis=0, keepdims=True)

    def exchange(box, which):
        return [
            pltpu.make_async_remote_copy(
                box.at[me], box.at[me], box_sem.at[2 * which], box_sem.at[2 * which + 1],
                device_id={"rows": peer(d)}, device_id_type=MESH,
            )
            for d in range(1, 8)
        ]

    def exchanged(box, which):
        return pltpu.make_async_remote_copy(
            box.at[pl.ds(0, 7)], box.at[pl.ds(0, 7)], box_sem.at[2 * which], box_sem.at[2 * which + 1],
            device_id={"rows": sibling}, device_id_type=MESH,
        )

    def piece(m, owner, k):
        return outs[m].at[pl.ds(pl.multiple_of(owner * rows + k * height, 16), height), :]

    def copy(m, owner, k, stream, target):
        ref = piece(m, owner, k)
        arrive = {OWN_X: x_sem, OWN_Y: y_sem, DIAG: d_sem}.get(stream)
        arrive = bulk_sem.at[m, stream] if arrive is None else arrive.at[m, k]
        return pltpu.make_async_remote_copy(
            ref, ref, send_sem.at[m, stream], arrive,
            device_id={"rows": target}, device_id_type=MESH,
        )

    def whole(m, stream):
        ref = outs[m].at[pl.ds(0, rows), :]
        return pltpu.make_async_remote_copy(
            ref, ref, send_sem.at[m, stream], bulk_sem.at[m, stream],
            device_id={"rows": sibling}, device_id_type=MESH,
        )

    def narrow(m, k, inverse):
        def body(i, _):
            at = pl.multiple_of(k * height + i * 16, 16)
            small = (held[2 * m, pl.ds(at, 16), :] * inverse).astype(jnp.bfloat16)
            outs[m][pl.ds(pl.multiple_of(me * rows + at, 16), 16), :] = small
            return 0

        lax.fori_loop(0, height // 16, body, 0, unroll=True)

    def send_own(m, k):
        copy(m, me, k, OWN_X, at_x).start()
        copy(m, me, k, OWN_Y, at_y).start()
        copy(m, me, k, OWN_S, sibling).start()

    box_first[me] = mix(0)
    pl.semaphore_wait(barrier, 7)
    for c in exchange(box_first, 0):
        c.start()
    exchanged(box_first, 0).wait_recv()
    factor = jnp.max(box_first[...], axis=0)
    factors[0] = factor
    inverse = 1.0 / factor
    for k in range(chunks):
        narrow(0, k, inverse)
        if 1 <= k <= half:
            send_own(0, k - 1)

    box_rest[me, 0:1] = mix(1)
    box_rest[me, 1:2] = mix(2)
    for c in exchange(box_rest, 1):
        c.start()
    for k in range(half, chunks):
        send_own(0, k)
    exchanged(box_rest, 1).wait_recv()
    both = jnp.max(box_rest[...], axis=0)
    for m in (1, 2):
        factor = both[m - 1:m]
        factors[m] = factor
        inverse = 1.0 / factor
        for k in range(chunks):
            narrow(m, k, inverse)
            if k:
                send_own(m, k - 1)
        send_own(m, chunks - 1)

    for m in range(3):
        for k in range(chunks):
            copy(m, at_x, k, OWN_X, at_x).wait_recv()
            copy(m, at_x, k, X_S, sibling).start()
            if k < half:
                copy(m, at_x, k, DIAG, at_y).start()
            copy(m, at_y, k, OWN_Y, at_y).wait_recv()
            copy(m, at_y, k, Y_S, sibling).start()
            if k >= half:
                copy(m, at_y, k, DIAG, at_x).start()
    for m in range(3):
        for k in range(half):
            for part in (k, k + half):
                copy(m, at_d, part, DIAG, at_y).wait_recv()
                copy(m, at_d, part, D_S, sibling).start()

    for m in range(3):
        for stream in (OWN_S, X_S, Y_S, D_S):
            whole(m, stream).wait_recv()
    for m in range(3):
        for stream in range(7):
            whole(m, stream).wait_send()
    exchanged(box_first, 0).wait_send()
    exchanged(box_rest, 1).wait_send()


def settle(factors, gathered, *refs):
    targets, sems = refs[:6], refs[6]
    parts = sems.shape[1]
    height = gathered.shape[1] // parts
    copies = [
        pltpu.make_async_copy(
            gathered.at[m, pl.ds(p * height, height), :],
            targets[m].at[pl.ds(p * height, height), :],
            sems.at[m, p],
        )
        for p in range(parts)
        for m in range(3)
    ]
    for c in copies:
        c.start()
    for m in range(3):
        targets[3 + m][...] = factors[m, 0]
    for c in copies:
        c.wait()


def gathered_by_kernel(*arrays):
    *weights, mix_share, norm_gain = arrays
    rows, columns = weights[0].shape
    chunks = 8
    vmem, hbm = pl.BlockSpec(memory_space=pltpu.VMEM), pl.BlockSpec(memory_space=pltpu.HBM)
    dma = pltpu.SemaphoreType.DMA
    results = pl.pallas_call(
        functools.partial(kernel, chunks),
        out_shape=[
            pltpu.VMEM((3, 1, columns), jnp.float32),
            pltpu.VMEM((3, 8 * rows, columns), jnp.bfloat16),
        ],
        in_specs=[vmem] * 2 + [hbm] * 6,
        out_specs=[vmem] * 2,
        scratch_shapes=[
            pltpu.VMEM((6, rows, columns), jnp.float32),
            pltpu.VMEM((rows, LANES), jnp.float32),
            pltpu.VMEM((rows, LANES), jnp.float32),
            pltpu.VMEM((8, 1, columns), jnp.float32),
            pltpu.VMEM((8, 2, columns), jnp.float32),
            dma((6,)),
            dma((3, 7)),
            dma((3, 7)),
            dma((3, chunks)),
            dma((3, chunks)),
            dma((3, chunks)),
            dma((4,)),
        ],
        compiler_params=pltpu.CompilerParams(
            collective_id=0, has_side_effects=True, vmem_limit_bytes=22 * 2**20
        ),
    )(mix_share, norm_gain, *weights)
    results = [pltpu.with_memory_space_constraint(r, pltpu.VMEM) for r in results]
    return tuple(
        pl.pallas_call(
            settle,
            out_shape=[jax.ShapeDtypeStruct((8 * rows, columns), jnp.bfloat16)] * 3
            + [jax.ShapeDtypeStruct((columns,), jnp.float32)] * 3,
            in_specs=[vmem] * 2,
            out_specs=[pl.BlockSpec(memory_space=pl.ANY)] * 3 + [vmem] * 3,
            scratch_shapes=[dma((3, 8))],
            compiler_params=pltpu.CompilerParams(vmem_limit_bytes=2**20),
        )(*results)
    )


def solution(mesh):
    placed = (P("rows", "model"),) * 6 + (P("rows"),) * 2
    local = gathered_by_kernel if mesh.shape["rows"] == 8 else gathered_by_collectives
    return jax.shard_map(
        local,
        mesh=mesh,
        in_specs=placed,
        out_specs=(P(None, "model"),) * 3 + (P("model"),) * 3,
        check_vma=False,
    )
```
